32 devices in a mesh: node: 2 (over y), space: 16 (over z, x, core).
Axes of the slice: x: 2, y: 2, z: 4, core: 2. Of those that a mesh axis runs over, the one named last changes fastest.
Arguments:
- u_start: float32 [128, 256, 128], P('space'), may hold values from 0 to 1
- v_start: float32 [128, 256, 128], P('space'), may hold values from 0 to 2
- labels: int32 [128, 256, 128], P('space'), may hold values from 0 to 2
- u_guess: float32 [4, 128, 256, 128], P('node', 'space'), may hold values from 0 to 1
- v_guess: float32 [4, 128, 256, 128], P('node', 'space'), may hold values from 0 to 2
Outputs:
- u_nodes: float32 [4, 128, 256, 128], P('node', 'space')
- v_nodes: float32 [4, 128, 256, 128], P('node', 'space')
The draws below stay inside these ranges and needn't reach their ends.
Inputs may be any that keep to these rules, and one draw needn't show every extreme that they name: `labels`: 0 marks healthy, 1 fibrous and 2 scar tissue.
All inputs are finite; a program needn't handle non-finite values.
Results may differ from the reference program's by a relative error of at most 0.0001.
Values sent between devices are 32-bit elements; how exact they have to be, the bound alone decides.
A program may use at most 192 MiB of HBM per device.

```python
import jax
import jax.numpy as jnp
from jax import lax

NY = 256
NZ = 128
NODES = 4
SWEEPS = 2
NX = 128


def set_ends(result, rng, smallest, largest):
    longest = result.shape.index(max(result.shape))
    spots = []
    for shift in (0, 1):
        where = [jax.random.randint(jax.random.fold_in(rng, axis), (), 0, length) for axis, length in enumerate(result.shape)]
        where[longest] = (where[longest] + shift) % result.shape[longest]
        spots.append(tuple(where))
    return result.at[spots[0]].set(smallest).at[spots[1]].set(largest)


def levels(own_key, shape, split, smallest, top_value):
    def one(dim, shards_of):
        heights = jax.random.uniform(jax.random.fold_in(jax.random.fold_in(own_key, 6), dim), (shards_of,), jnp.float32, smallest / len(split), top_value / len(split))
        return jnp.repeat(jnp.exp(heights), shape[dim] // shards_of).reshape((-1,) + (1,) * (len(shape) - dim - 1))

    gain = one(*split[0])
    for cut in split[1:]:
        gain = gain * one(*cut)
    return gain


def setup_inputs(seed: int = 0) -> dict:
    seeds = jax.random.split(jax.random.key(seed), 6)
    return {
        "u_start": jnp.clip(1.0 * jax.random.uniform(seeds[0], (NX, NY, NZ), jnp.float32) ** levels(seeds[0], (NX, NY, NZ), ((0, 16),), -0.2, 0.2), 0.0, 1.0),
        "v_start": jnp.clip(2.0 * jax.random.uniform(seeds[1], (NX, NY, NZ), jnp.float32) ** levels(seeds[1], (NX, NY, NZ), ((0, 16),), -0.2, 0.2), 0.0, 2.0),
        "labels": set_ends(jax.random.randint(seeds[2], (NX, NY, NZ), 0, 3), jax.random.fold_in(seeds[2], 1), 0, 2).astype(jnp.int32),
        "u_guess": jnp.clip(1.0 * jax.random.uniform(seeds[3], (NODES, NX, NY, NZ), jnp.float32) ** levels(seeds[3], (NODES, NX, NY, NZ), ((0, 2), (1, 16)), -0.2, 0.2), 0.0, 1.0),
        "v_guess": jnp.clip(2.0 * jax.random.uniform(seeds[4], (NODES, NX, NY, NZ), jnp.float32) ** levels(seeds[4], (NODES, NX, NY, NZ), ((0, 2), (1, 16)), -0.2, 0.2), 0.0, 2.0),
    }


radau_points = (0.08858795951270395, 0.4094668644407347, 0.7876594617608471, 1.0)
time_step = 0.16
onset_level = 0.15
ionic_gain = 8.0
recovery_base = 0.002
recovery_slope = 0.2
recovery_offset = 0.3
conductances = (1.0, 0.35, 0.05)
excitability = (1.0, 0.6, 0.0)


def weight_table():
    table = []
    for target in range(4):
        entries = []
        for column in range(4):
            coeffs = [1.0]
            for other in range(4):
                if other != column:
                    factor = 1.0 / (radau_points[column] - radau_points[other])
                    raised = [0.0] + coeffs
                    lowered = coeffs + [0.0]
                    coeffs = [factor * (raised[place] - radau_points[other] * lowered[place]) for place in range(len(raised))]
            integral = 0.0
            for place in range(len(coeffs)):
                integral = integral + coeffs[place] * radau_points[target] ** (place + 1) / (place + 1)
            entries.append(time_step * integral)
        table.append(entries)
    return table


def label_values(labels, values):
    return jnp.where(labels == 0, jnp.float32(values[0]),
                     jnp.where(labels == 1, jnp.float32(values[1]), jnp.float32(values[2])))


def neighbours(field):
    padded = jnp.pad(field, 1)
    return (padded[2:, 1:-1, 1:-1], padded[:-2, 1:-1, 1:-1],
            padded[1:-1, 2:, 1:-1], padded[1:-1, :-2, 1:-1],
            padded[1:-1, 1:-1, 2:], padded[1:-1, 1:-1, :-2])


def rates(u_field, v_field, conduct, excite):
    conduct_sides = neighbours(conduct)
    voltage_sides = neighbours(u_field)
    spread = jnp.zeros_like(u_field)
    for conduct_side, voltage_side in zip(conduct_sides, voltage_sides):
        facing = 2.0 * conduct * conduct_side / (conduct + conduct_side)
        spread = spread + facing * (voltage_side - u_field)
    ionic = ionic_gain * u_field * (u_field - onset_level) * (1.0 - u_field) - u_field * v_field
    rate_u = spread + excite * ionic
    recovery = recovery_base + recovery_slope * v_field / jnp.maximum(u_field + recovery_offset, recovery_offset)
    rate_v = recovery * (-v_field - ionic_gain * u_field * (u_field - onset_level - 1.0))
    return rate_u, rate_v


def reference(u_start, v_start, labels, u_guess, v_guess):
    conduct = label_values(labels, conductances)
    excite = label_values(labels, excitability)
    weights = jnp.asarray(weight_table(), jnp.float32)
    u_nodes, v_nodes = u_guess, v_guess
    for sweep_index in range(SWEEPS):
        rate_u, rate_v = lax.map(lambda node_pair: rates(node_pair[0], node_pair[1], conduct, excite), (u_nodes, v_nodes))
        u_nodes = u_start[None] + jnp.einsum("ij,jabc->iabc", weights, rate_u, precision=lax.Precision.HIGHEST)
        v_nodes = v_start[None] + jnp.einsum("ij,jabc->iabc", weights, rate_v, precision=lax.Precision.HIGHEST)
    return u_nodes, v_nodes
```

```python
import functools

import jax
import jax.numpy as jnp
from jax import lax
from jax.experimental import pallas as pl
from jax.experimental.pallas import tpu as pltpu
from jax.sharding import PartitionSpec as P

SWEEPS = 2


radau_points = (0.08858795951270396, 0.4094668644407347, 0.7876594617608471, 1.0)
time_step = 0.16
onset_level = 0.15
ionic_gain = 8.0
recovery_base = 0.002
recovery_slope = 0.2
recovery_offset = 0.3
conductances = (1.0, 0.35, 0.05)
excitability = (1.0, 0.6, 0.0)


def weight_table():
    table = []
    for target in range(4):
        entries = []
        for column in range(4):
            coeffs = [1.0]
            for other in range(4):
                if other != column:
                    factor = 1.0 / (radau_points[column] - radau_points[other])
                    raised = [0.0] + coeffs
                    lowered = coeffs + [0.0]
                    coeffs = [
                        factor * (raised[place] - radau_points[other] * lowered[place])
                        for place in range(len(raised))
                    ]
            integral = 0.0
            for place in range(len(coeffs)):
                integral = integral + coeffs[place] * radau_points[target] ** (place + 1) / (
                    place + 1
                )
            entries.append(time_step * integral)
        table.append(entries)
    return table


def label_values(labels, values):
    return jnp.where(
        labels == 0,
        jnp.float32(values[0]),
        jnp.where(labels == 1, jnp.float32(values[1]), jnp.float32(values[2])),
    )


MESH = pl.DeviceIdType.MESH
PAD = 8
ROWS = 16
LAST_ROWS = 32


def kernel(
    node_count, space_count, u_start, v_start, labels, u_guess, v_guess, u_out, v_out,
    u_old, u_new, v_now, u_first, v_first, lab, conduct, face_x, face_y, face_z, excite,
    load_sem, side_send, side_recv, guess_send, guess_recv, v_send, v_recv,
):
    own, planes, height, width = u_guess.shape
    total = own * node_count
    me, place = lax.axis_index("node"), lax.axis_index("space")
    peer = 1 - me
    right = lax.rem(place + 1, space_count)
    left = lax.rem(place + space_count - 1, space_count)
    mine, theirs = pl.ds(me * own, own), pl.ds(peer * own, own)
    inner = pl.ds(PAD, height)
    weights = weight_table()
    last = planes - 2
    order = [0, planes - 1] + list(range(1, last))
    last_tiles = height // LAST_ROWS

    barrier = pltpu.get_barrier_semaphore()
    for target in ({"node": peer}, {"space": left}, {"space": right}):
        pl.semaphore_signal(barrier, inc=1, device_id=target, device_id_type=MESH)

    loads = [
        pltpu.make_async_copy(source, target, load_sem.at[index])
        for index, (source, target) in enumerate((
            (labels, lab.at[pl.ds(1, planes)]),
            (u_guess, u_old.at[mine, pl.ds(1, planes), inner]),
            (v_guess, v_now.at[mine]),
            (u_start, u_first),
            (v_start, v_first),
        ))
    ]
    for load in loads:
        load.start()
    pl.semaphore_wait(barrier, 3)

    def remote(source, target, send, recv, device):
        return pltpu.make_async_remote_copy(
            src_ref=source, dst_ref=target, send_sem=send, recv_sem=recv,
            device_id=device, device_id_type=MESH,
        )

    def side(index, source, target, device):
        return remote(source, target, side_send.at[index], side_recv.at[index], {"space": device})

    def guess(index, first, count):
        return remote(
            u_guess.at[:, pl.ds(first, count)],
            u_old.at[mine, pl.ds(first + 1, count), inner],
            guess_send.at[index], guess_recv.at[index], {"node": peer},
        )

    def recovery_plane(index, plane):
        return remote(
            v_guess.at[:, plane], v_now.at[mine, plane],
            v_send.at[index], v_recv.at[index], {"node": peer},
        )

    def recovery_tile(tile):
        rows = pl.ds(pl.multiple_of(tile * LAST_ROWS, LAST_ROWS), LAST_ROWS)
        index = len(order) + tile
        return remote(
            v_guess.at[:, last, rows], v_now.at[mine, last, rows],
            v_send.at[index], v_recv.at[index], {"node": peer},
        )

    guesses = [guess(0, 0, 1), guess(1, planes - 1, 1), guess(2, 1, planes - 2)]
    recoveries = [recovery_plane(index, plane) for index, plane in enumerate(order)]
    label_sides = [
        side(0, labels.at[planes - 1], lab.at[0], right),
        side(1, labels.at[0], lab.at[planes + 1], left),
    ]
    own_sides = [
        side(2, u_guess.at[:, planes - 1], u_old.at[mine, 0, inner], right),
        side(3, u_guess.at[:, 0], u_old.at[mine, planes + 1, inner], left),
    ]
    for copy in guesses + label_sides + own_sides + recoveries:
        copy.start()

    @pl.loop(0, last_tiles)
    def _(tile):
        recovery_tile(tile).start()

    edge = jnp.zeros((PAD, width), jnp.float32)
    for field in (u_old, u_new):
        for node in range(total):
            for plane in range(1, planes + 1):
                field[node, plane, 0:PAD] = edge
                field[node, plane, PAD + height : PAD + height + PAD] = edge
    for plane in range(planes):
        face_y[plane, 0:PAD] = edge
        conduct[plane + 1, 0:PAD] = edge
        conduct[plane + 1, PAD + height : PAD + height + PAD] = edge

    loads[0].wait()
    for copy in label_sides:
        copy.wait()

    @pl.loop(0, planes + 2)
    def _(plane):
        outside = ((plane == 0) & (place == 0)) | (
            (plane == planes + 1) & (place == space_count - 1)
        )
        scale = jnp.where(outside, jnp.float32(0), jnp.float32(1))

        @pl.loop(0, height // ROWS)
        def _(step):
            row = pl.multiple_of(step * ROWS, ROWS)
            found = label_values(lab[plane, pl.ds(row, ROWS)], conductances)
            conduct[plane, pl.ds(row + PAD, ROWS)] = found * scale

    def face(one, other):
        return 2.0 * one * other / (one + other)

    @pl.loop(0, planes + 1)
    def _(plane):
        @pl.loop(0, height // ROWS)
        def _(step):
            row = pl.multiple_of(step * ROWS, ROWS)
            here = conduct[plane, pl.ds(row + PAD, ROWS)]
            face_x[plane, pl.ds(row, ROWS)] = face(here, conduct[plane + 1, pl.ds(row + PAD, ROWS)])

    @pl.loop(0, planes)
    def _(plane):
        @pl.loop(0, height // ROWS)
        def _(step):
            row = pl.multiple_of(step * ROWS, ROWS)
            here = conduct[plane + 1, pl.ds(row + PAD, ROWS)]
            face_y[plane, pl.ds(row + PAD, ROWS)] = face(
                here, conduct[plane + 1, pl.ds(row + PAD + 1, ROWS)]
            )
            beside = face(here, pltpu.roll(here, width - 1, 1))
            lane = lax.broadcasted_iota(jnp.int32, (ROWS, width), 1)
            face_z[plane, pl.ds(row, ROWS)] = jnp.where(lane == width - 1, 0.0, beside)
            excite[plane, pl.ds(row, ROWS)] = label_values(
                lab[plane + 1, pl.ds(row, ROWS)], excitability
            )

    loads[1].wait()
    guesses[0].wait_recv()
    relays = [side(4, u_old.at[theirs, 1, inner], u_old.at[theirs, planes + 1, inner], left)]
    relays[0].start()
    guesses[1].wait_recv()
    relays.append(side(5, u_old.at[theirs, planes, inner], u_old.at[theirs, 0, inner], right))
    relays[1].start()
    for load in loads[2:]:
        load.wait()
    for copy in own_sides + relays:
        copy.wait()
    guesses[2].wait_recv()

    def sweep(field, plane, first_row, count, table, write):
        @pl.loop(0, count // ROWS)
        def _(step):
            row = pl.multiple_of(first_row + step * ROWS, ROWS)
            rows = pl.ds(row, ROWS)
            mid = pl.ds(row + PAD, ROWS)
            up, down = pl.ds(row + PAD + 1, ROWS), pl.ds(row + PAD - 1, ROWS)
            x_high, x_low = face_x[plane + 1, rows], face_x[plane, rows]
            y_high, y_low = face_y[plane, mid], face_y[plane, down]
            z_high = face_z[plane, rows]
            active = excite[plane, rows]
            sums_u = [u_first[plane, rows]] * len(table)
            sums_v = [v_first[plane, rows]] * len(table)
            for node in range(total):
                u = field[node, plane + 1, mid]
                v = v_now[node, plane, rows]
                flux = z_high * (pltpu.roll(u, width - 1, 1) - u)
                spread = flux - pltpu.roll(flux, 1, 1)
                spread += x_high * (field[node, plane + 2, mid] - u)
                spread += x_low * (field[node, plane, mid] - u)
                spread += y_high * (field[node, plane + 1, up] - u)
                spread += y_low * (field[node, plane + 1, down] - u)
                gained = ionic_gain * u
                ionic = gained * (u - onset_level) * (1.0 - u) - u * v
                rate_u = spread + active * ionic
                recovery = recovery_base + recovery_slope * v / jnp.maximum(
                    u + recovery_offset, recovery_offset
                )
                rate_v = recovery * (-v - gained * (u - onset_level - 1.0))
                for target in range(len(table)):
                    sums_u[target] = sums_u[target] + table[target][node] * rate_u
                    sums_v[target] = sums_v[target] + table[target][node] * rate_v
            for target in range(len(table)):
                write(target, plane, row, sums_u[target], sums_v[target])

    def write_first(target, plane, row, u, v):
        u_new[target, plane + 1, pl.ds(row + PAD, ROWS)] = u
        v_now[target, plane, pl.ds(row, ROWS)] = v

    def write_second(target, plane, row, u, v):
        u_out[target, plane, pl.ds(row, ROWS)] = u
        v_out[target, plane, pl.ds(row, ROWS)] = v

    table_first = [[jnp.float32(value) for value in line] for line in weights]
    table_second = []
    for target in range(own):
        line = []
        for node in range(total):
            value = jnp.float32(weights[target][node])
            for rank in range(1, node_count):
                value = jnp.where(me == rank, jnp.float32(weights[rank * own + target][node]), value)
            line.append(value)
        table_second.append(line)

    def first(plane, row=0, count=height):
        sweep(u_old, plane, row, count, table_first, write_first)

    def second(plane, row=0, count=height):
        sweep(u_new, plane, row, count, table_second, write_second)

    new_sides = [
        side(6, u_new.at[:, 1, inner], u_new.at[:, planes + 1, inner], left),
        side(7, u_new.at[:, planes, inner], u_new.at[:, 0, inner], right),
    ]
    for index, plane in enumerate(order):
        recoveries[index].wait_recv()
        first(plane)
        if plane == 1:
            for copy in new_sides:
                copy.start()
        if 2 <= plane < planes - 1:
            second(plane - 1)
        if plane == planes - 4:
            new_sides[0].wait_recv()
            new_sides[1].wait_recv()
            second(0)

    @pl.loop(0, last_tiles)
    def _(tile):
        recovery_tile(tile).wait_recv()
        row = pl.multiple_of(tile * LAST_ROWS, LAST_ROWS)
        first(last, row, LAST_ROWS)
        second(last - 1, row, LAST_ROWS)
        second(planes - 1, row, LAST_ROWS)

        @pl.when(tile > 0)
        def _():
            second(last, pl.multiple_of(row - LAST_ROWS, LAST_ROWS), LAST_ROWS)

    second(last, height - LAST_ROWS, LAST_ROWS)

    for copy in guesses + new_sides + recoveries:
        copy.wait_send()

    @pl.loop(0, last_tiles)
    def _(tile):
        recovery_tile(tile).wait_send()


def on_device(mesh, u_start, v_start, labels, u_guess, v_guess):
    own, planes, height, width = u_guess.shape
    node_count, space_count = mesh.shape["node"], mesh.shape["space"]
    assert node_count == 2
    total = own * node_count
    padded = (planes + 2, height + 2 * PAD, width)
    slab = (planes, height, width)
    copies = planes - 1 + height // LAST_ROWS
    result = jax.ShapeDtypeStruct(u_guess.shape, jnp.float32)
    dma = pltpu.SemaphoreType.DMA
    f32 = jnp.float32
    return pl.pallas_call(
        functools.partial(kernel, node_count, space_count),
        out_shape=(result, result),
        in_specs=[pl.BlockSpec(memory_space=pl.ANY)] * 5,
        out_specs=(pl.BlockSpec(memory_space=pltpu.VMEM),) * 2,
        scratch_shapes=[
            pltpu.VMEM((total,) + padded, f32),
            pltpu.VMEM((total,) + padded, f32),
            pltpu.VMEM((total,) + slab, f32),
            pltpu.VMEM(slab, f32),
            pltpu.VMEM(slab, f32),
            pltpu.VMEM((planes + 2, height, width), jnp.int32),
            pltpu.VMEM(padded, f32),
            pltpu.VMEM((planes + 1, height, width), f32),
            pltpu.VMEM((planes, height + 2 * PAD, width), f32),
            pltpu.VMEM(slab, f32),
            pltpu.VMEM(slab, f32),
            dma((5,)), dma((8,)), dma((8,)), dma((3,)), dma((3,)), dma((copies,)), dma((copies,)),
        ],
        compiler_params=pltpu.CompilerParams(collective_id=0, has_side_effects=True),
    )(u_start, v_start, labels, u_guess, v_guess)


def solution(mesh):
    return jax.shard_map(
        functools.partial(on_device, mesh),
        mesh=mesh,
        in_specs=(
            P("space", None, None),
            P("space", None, None),
            P("space", None, None),
            P("node", "space", None, None),
            P("node", "space", None, None),
        ),
        out_specs=(P("node", "space", None, None), P("node", "space", None, None)),
        check_vma=False,
    )
```

```python
import functools

import jax
import jax.numpy as jnp
from jax import lax
from jax.experimental import pallas as pl
from jax.experimental.pallas import tpu as pltpu
from jax.sharding import PartitionSpec as P

SWEEPS = 2


radau_points = (0.08858795951270396, 0.4094668644407347, 0.7876594617608471, 1.0)
time_step = 0.16
onset_level = 0.15
ionic_gain = 8.0
recovery_base = 0.002
recovery_slope = 0.2
recovery_offset = 0.3
conductances = (1.0, 0.35, 0.05)
excitability = (1.0, 0.6, 0.0)


def weight_table():
    table = []
    for target in range(4):
        entries = []
        for column in range(4):
            coeffs = [1.0]
            for other in range(4):
                if other != column:
                    factor = 1.0 / (radau_points[column] - radau_points[other])
                    raised = [0.0] + coeffs
                    lowered = coeffs + [0.0]
                    coeffs = [
                        factor * (raised[place] - radau_points[other] * lowered[place])
                        for place in range(len(raised))
                    ]
            integral = 0.0
            for place in range(len(coeffs)):
                integral = integral + coeffs[place] * radau_points[target] ** (place + 1) / (
                    place + 1
                )
            entries.append(time_step * integral)
        table.append(entries)
    return table


def label_values(labels, values):
    return jnp.where(
        labels == 0,
        jnp.float32(values[0]),
        jnp.where(labels == 1, jnp.float32(values[1]), jnp.float32(values[2])),
    )


MESH = pl.DeviceIdType.MESH
PAD = 8
ROWS = 16
VMEM_LIMIT = 46 * 2**20
LAST_ROWS = 64
WINDOW = 5
TILE_WINDOW = 4


def kernel(
    node_count, space_count, u_start, v_start, labels, u_guess, v_guess, u_out, v_out,
    u_old, u_new, v_now, u_first, v_first, lab, conduct, face_x, face_y, face_z, excite,
    load_sem, side_send, side_recv, guess_send, guess_recv, v_send, v_recv,
):
    own, planes, height, width = u_guess.shape
    total = own * node_count
    me, place = lax.axis_index("node"), lax.axis_index("space")
    peer = 1 - me
    right = lax.rem(place + 1, space_count)
    left = lax.rem(place + space_count - 1, space_count)
    mine, theirs = pl.ds(me * own, own), pl.ds(peer * own, own)
    inner = pl.ds(PAD, height)
    weights = weight_table()
    last = planes - 2
    order = [0, planes - 1] + list(range(1, last))
    last_tiles = height // LAST_ROWS

    barrier = pltpu.get_barrier_semaphore()
    for target in ({"node": peer}, {"space": left}, {"space": right}):
        pl.semaphore_signal(barrier, inc=1, device_id=target, device_id_type=MESH)

    loads = [
        pltpu.make_async_copy(source, target, load_sem.at[index])
        for index, (source, target) in enumerate((
            (labels, lab.at[pl.ds(1, planes)]),
            (u_guess, u_old.at[mine, pl.ds(1, planes), inner]),
            (v_guess, v_now.at[mine]),
            (u_start, u_first),
            (v_start, v_first),
        ))
    ]
    for load in loads:
        load.start()
    pl.semaphore_wait(barrier, 3)

    def remote(source, target, send, recv, device):
        return pltpu.make_async_remote_copy(
            src_ref=source, dst_ref=target, send_sem=send, recv_sem=recv,
            device_id=device, device_id_type=MESH,
        )

    def side(index, source, target, device):
        return remote(source, target, side_send.at[index], side_recv.at[index], {"space": device})

    def guess(index, first, count):
        return remote(
            u_guess.at[:, pl.ds(first, count)],
            u_old.at[mine, pl.ds(first + 1, count), inner],
            guess_send.at[index], guess_recv.at[index], {"node": peer},
        )

    def recovery_plane(index, plane):
        return remote(
            v_guess.at[:, plane], v_now.at[mine, plane],
            v_send.at[index], v_recv.at[index], {"node": peer},
        )

    def recovery_tile(tile):
        rows = pl.ds(pl.multiple_of(tile * LAST_ROWS, LAST_ROWS), LAST_ROWS)
        index = len(order) + tile
        return remote(
            v_guess.at[:, last, rows], v_now.at[mine, last, rows],
            v_send.at[index], v_recv.at[index], {"node": peer},
        )

    guesses = [guess(0, 0, 1), guess(1, planes - 1, 1), guess(2, 1, planes - 2)]
    recoveries = [recovery_plane(index, plane) for index, plane in enumerate(order)]
    label_sides = [
        side(0, labels.at[planes - 1], lab.at[0], right),
        side(1, labels.at[0], lab.at[planes + 1], left),
    ]
    own_sides = [
        side(2, u_guess.at[:, planes - 1], u_old.at[mine, 0, inner], right),
        side(3, u_guess.at[:, 0], u_old.at[mine, planes + 1, inner], left),
    ]
    queue = guesses + recoveries + [recovery_tile(tile) for tile in range(TILE_WINDOW)]

    def advance(count=1):
        for copy in queue[:count]:
            copy.start()
        del queue[:count]

    advance(WINDOW)
    for copy in label_sides + own_sides:
        copy.start()

    edge = jnp.zeros((PAD, width), jnp.float32)
    for field in (u_old, u_new):
        for node in range(total):
            for plane in range(1, planes + 1):
                field[node, plane, 0:PAD] = edge
                field[node, plane, PAD + height : PAD + height + PAD] = edge
    for plane in range(planes):
        face_y[plane, 0:PAD] = edge
        conduct[plane + 1, 0:PAD] = edge
        conduct[plane + 1, PAD + height : PAD + height + PAD] = edge

    loads[0].wait()
    for copy in label_sides:
        copy.wait()

    @pl.loop(0, planes + 2)
    def _(plane):
        outside = ((plane == 0) & (place == 0)) | (
            (plane == planes + 1) & (place == space_count - 1)
        )
        scale = jnp.where(outside, jnp.float32(0), jnp.float32(1))

        @pl.loop(0, height // ROWS)
        def _(step):
            row = pl.multiple_of(step * ROWS, ROWS)
            found = label_values(lab[plane, pl.ds(row, ROWS)], conductances)
            conduct[plane, pl.ds(row + PAD, ROWS)] = found * scale

    def face(one, other):
        return 2.0 * one * other / (one + other)

    @pl.loop(0, planes + 1)
    def _(plane):
        @pl.loop(0, height // ROWS)
        def _(step):
            row = pl.multiple_of(step * ROWS, ROWS)
            here = conduct[plane, pl.ds(row + PAD, ROWS)]
            face_x[plane, pl.ds(row, ROWS)] = face(here, conduct[plane + 1, pl.ds(row + PAD, ROWS)])

    @pl.loop(0, planes)
    def _(plane):
        @pl.loop(0, height // ROWS)
        def _(step):
            row = pl.multiple_of(step * ROWS, ROWS)
            here = conduct[plane + 1, pl.ds(row + PAD, ROWS)]
            face_y[plane, pl.ds(row + PAD, ROWS)] = face(
                here, conduct[plane + 1, pl.ds(row + PAD + 1, ROWS)]
            )
            beside = face(here, pltpu.roll(here, width - 1, 1))
            lane = lax.broadcasted_iota(jnp.int32, (ROWS, width), 1)
            face_z[plane, pl.ds(row, ROWS)] = jnp.where(lane == width - 1, 0.0, beside)
            excite[plane, pl.ds(row, ROWS)] = label_values(
                lab[plane + 1, pl.ds(row, ROWS)], excitability
            )

    loads[1].wait()
    guesses[0].wait_recv()
    relays = [side(4, u_old.at[theirs, 1, inner], u_old.at[theirs, planes + 1, inner], left)]
    relays[0].start()
    guesses[1].wait_recv()
    relays.append(side(5, u_old.at[theirs, planes, inner], u_old.at[theirs, 0, inner], right))
    relays[1].start()
    for load in loads[2:]:
        load.wait()
    for copy in own_sides + relays:
        copy.wait()
    guesses[2].wait_recv()
    advance()

    def sweep(field, plane, first_row, count, table, write):
        @pl.loop(0, count // ROWS)
        def _(step):
            row = pl.multiple_of(first_row + step * ROWS, ROWS)
            rows = pl.ds(row, ROWS)
            mid = pl.ds(row + PAD, ROWS)
            up, down = pl.ds(row + PAD + 1, ROWS), pl.ds(row + PAD - 1, ROWS)
            x_high, x_low = face_x[plane + 1, rows], face_x[plane, rows]
            y_high, y_low = face_y[plane, mid], face_y[plane, down]
            z_high = face_z[plane, rows]
            active = excite[plane, rows]
            sums_u = [u_first[plane, rows]] * len(table)
            sums_v = [v_first[plane, rows]] * len(table)
            for node in range(total):
                u = field[node, plane + 1, mid]
                v = v_now[node, plane, rows]
                flux = z_high * (pltpu.roll(u, width - 1, 1) - u)
                spread = flux - pltpu.roll(flux, 1, 1)
                spread += x_high * (field[node, plane + 2, mid] - u)
                spread += x_low * (field[node, plane, mid] - u)
                spread += y_high * (field[node, plane + 1, up] - u)
                spread += y_low * (field[node, plane + 1, down] - u)
                gained = ionic_gain * u
                ionic = gained * (u - onset_level) * (1.0 - u) - u * v
                rate_u = spread + active * ionic
                recovery = recovery_base + recovery_slope * v / jnp.maximum(
                    u + recovery_offset, recovery_offset
                )
                rate_v = recovery * (-v - gained * (u - onset_level - 1.0))
                for target in range(len(table)):
                    sums_u[target] = sums_u[target] + table[target][node] * rate_u
                    sums_v[target] = sums_v[target] + table[target][node] * rate_v
            for target in range(len(table)):
                write(target, plane, row, sums_u[target], sums_v[target])

    def write_first(target, plane, row, u, v):
        u_new[target, plane + 1, pl.ds(row + PAD, ROWS)] = u
        v_now[target, plane, pl.ds(row, ROWS)] = v

    def write_second(target, plane, row, u, v):
        u_out[target, plane, pl.ds(row, ROWS)] = u
        v_out[target, plane, pl.ds(row, ROWS)] = v

    table_first = [[jnp.float32(value) for value in line] for line in weights]
    table_second = []
    for target in range(own):
        line = []
        for node in range(total):
            value = jnp.float32(weights[target][node])
            for rank in range(1, node_count):
                value = jnp.where(me == rank, jnp.float32(weights[rank * own + target][node]), value)
            line.append(value)
        table_second.append(line)

    def first(plane, row=0, count=height):
        sweep(u_old, plane, row, count, table_first, write_first)

    def second(plane, row=0, count=height):
        sweep(u_new, plane, row, count, table_second, write_second)

    new_sides = [
        side(6, u_new.at[:, 1, inner], u_new.at[:, planes + 1, inner], left),
        side(7, u_new.at[:, planes, inner], u_new.at[:, 0, inner], right),
    ]
    for index, plane in enumerate(order):
        recoveries[index].wait_recv()
        advance(1 if index + 1 < len(order) else len(queue))
        first(plane)
        if plane == 1:
            for copy in new_sides:
                copy.start()
        if 2 <= plane < planes - 1:
            second(plane - 1)
        if plane == planes - 4:
            new_sides[0].wait_recv()
            new_sides[1].wait_recv()
            second(0)

    @pl.loop(0, last_tiles)
    def _(tile):
        recovery_tile(tile).wait_recv()

        @pl.when(tile + TILE_WINDOW < last_tiles)
        def _():
            recovery_tile(tile + TILE_WINDOW).start()

        row = pl.multiple_of(tile * LAST_ROWS, LAST_ROWS)
        first(last, row, LAST_ROWS)
        second(last - 1, row, LAST_ROWS)
        second(planes - 1, row, LAST_ROWS)

        @pl.when(tile > 0)
        def _():
            second(last, pl.multiple_of(row - LAST_ROWS, LAST_ROWS), LAST_ROWS)

    second(last, height - LAST_ROWS, LAST_ROWS)

    for copy in guesses + new_sides + recoveries:
        copy.wait_send()

    @pl.loop(0, last_tiles)
    def _(tile):
        recovery_tile(tile).wait_send()


def on_device(mesh, u_start, v_start, labels, u_guess, v_guess):
    own, planes, height, width = u_guess.shape
    node_count, space_count = mesh.shape["node"], mesh.shape["space"]
    assert node_count == 2
    total = own * node_count
    padded = (planes + 2, height + 2 * PAD, width)
    slab = (planes, height, width)
    copies = planes - 1 + height // LAST_ROWS
    result = jax.ShapeDtypeStruct(u_guess.shape, jnp.float32)
    dma = pltpu.SemaphoreType.DMA
    f32 = jnp.float32
    return pl.pallas_call(
        functools.partial(kernel, node_count, space_count),
        out_shape=(result, result),
        in_specs=[pl.BlockSpec(memory_space=pltpu.HBM)] * 5,
        out_specs=(pl.BlockSpec(memory_space=pltpu.VMEM),) * 2,
        scratch_shapes=[
            pltpu.VMEM((total,) + padded, f32),
            pltpu.VMEM((total,) + padded, f32),
            pltpu.VMEM((total,) + slab, f32),
            pltpu.VMEM(slab, f32),
            pltpu.VMEM(slab, f32),
            pltpu.VMEM((planes + 2, height, width), jnp.int32),
            pltpu.VMEM(padded, f32),
            pltpu.VMEM((planes + 1, height, width), f32),
            pltpu.VMEM((planes, height + 2 * PAD, width), f32),
            pltpu.VMEM(slab, f32),
            pltpu.VMEM(slab, f32),
            dma((5,)), dma((8,)), dma((8,)), dma((3,)), dma((3,)), dma((copies,)), dma((copies,)),
        ],
        compiler_params=pltpu.CompilerParams(
            collective_id=0, has_side_effects=True, vmem_limit_bytes=VMEM_LIMIT
        ),
    )(u_start, v_start, labels, u_guess, v_guess)


def solution(mesh):
    return jax.shard_map(
        functools.partial(on_device, mesh),
        mesh=mesh,
        in_specs=(
            P("space", None, None),
            P("space", None, None),
            P("space", None, None),
            P("node", "space", None, None),
            P("node", "space", None, None),
        ),
        out_specs=(P("node", "space", None, None), P("node", "space", None, None)),
        check_vma=False,
    )
```
